128 devices in a mesh: dev: 128 (over z, x, y, core).
Axes of the slice: x: 4, y: 4, z: 4, core: 2. Of those that a mesh axis runs over, the one named last changes fastest.
Arguments:
- embeddings: bfloat16 [131072, 128], P('dev'), may hold values from -6 to 6
- ranks: int32 [131072], P('dev'), may hold values from 0 to 131071, as said below
- pair_weight: bfloat16 [256, 128], replicated, may hold values from -0.375 to 0.375
- pair_bias: float32 [128], replicated, may hold values from -3 to 3
- score_weight: bfloat16 [128], replicated, may hold values from -0.5 to 0.5
Outputs:
- scores: float32 [31, 131072], P(None, 'dev')
The draws below stay inside these ranges and needn't reach their ends.
Inputs may be any that keep to these rules, and one draw needn't show every extreme that they name: ranks is a permutation of 0 .. 131071. Of the records of one device, at most 16 have ranks in any one range [o * 1024, (o + 1) * 1024); on every device some range holds exactly 16 of them, and every range holds exactly 16 of some device's records.
All inputs are finite; a program needn't handle non-finite values.
Results may differ from the reference program's by a relative error of at most 0.0045.
Values may be sent and summed in bfloat16 or wider, within the bound.
A program may use at most 64 MiB of HBM per device.

```python
import jax
import jax.numpy as jnp
from jax import lax

E = 128
H = 128
WIN = 32
ROWS_DEV = 1024
NTOTAL = 131072


def draw_ranks(key, part):
    devices = NTOTAL // ROWS_DEV
    average = ROWS_DEV // devices
    base = jax.random.fold_in(key, 7919)
    key_owner, key_weight, key_rows, key_mix = jax.random.split(base, 4)
    owner_order = jax.random.permutation(key_owner, devices).astype(jnp.int32)
    halves = devices // 2 - 1
    lower = jax.random.randint(key_weight, (halves,), 0, 2 * average + 1).astype(jnp.int32)
    paired = jnp.stack([lower, 2 * average - lower], axis=1).reshape(-1)
    weights = jnp.concatenate([jnp.full((1,), 2 * average, jnp.int32), paired])
    bounds = jnp.cumsum(weights)
    slot_ids = jnp.arange(ROWS_DEV, dtype=jnp.int32)
    shifts = jnp.searchsorted(bounds, slot_ids, side='right').astype(jnp.int32)
    sources = jnp.arange(devices, dtype=jnp.int32)[:, None]
    owners = owner_order[(sources + shifts[None, :]) % devices]
    row_keys = jax.random.split(key_rows, devices)
    shuffles = jax.vmap(lambda one_key: jax.random.permutation(one_key, ROWS_DEV).astype(jnp.int32))(row_keys)
    owners = jnp.take_along_axis(owners, shuffles, axis=1)
    flat_owner = owners.reshape(-1)
    mixed = jax.random.permutation(key_mix, NTOTAL).astype(jnp.int32)
    placed = mixed[jnp.argsort(flat_owner[mixed], stable=True)]
    return jnp.zeros((NTOTAL,), jnp.int32).at[placed].set(jnp.arange(NTOTAL, dtype=jnp.int32))


def block_scale(key, shape, cuts, smallest, high):
    level, own = 1.0, jax.random.fold_in(key, 6)
    for dim, parts in cuts:
        heights = jnp.exp(jax.random.uniform(jax.random.fold_in(own, dim), (parts,), jnp.float32, smallest / len(cuts), high / len(cuts)))
        level = level * jnp.repeat(heights, shape[dim] // parts).reshape([-1 if axis == dim else 1 for axis in range(len(shape))])
    return level


def normal_values(key, shape, deviation, limit, pieces=(), kind=jnp.bfloat16):
    entries = deviation * jax.random.normal(key, shape, jnp.float32)
    if pieces:
        entries = entries * block_scale(key, shape, pieces, -0.22, 0.18)
    return jnp.clip(entries, -limit, limit).astype(kind)


def setup_inputs(seed: int = 0) -> dict:
    streams_of = jax.random.split(jax.random.key(seed), 6)
    embeddings = normal_values(streams_of[0], (NTOTAL, E), 1.0, 6.0, ((0, 128),))
    ranks = draw_ranks(jax.random.fold_in(streams_of[5], 71), 0)
    pair_weight = normal_values(streams_of[2], (2 * E, H), (2 * E) ** -0.5, 0.375)
    pair_bias = normal_values(streams_of[3], (H,), 0.5, 3.0, (), jnp.float32)
    score_weight = normal_values(streams_of[4], (H,), H ** -0.5, 0.5)
    return dict(embeddings=embeddings, ranks=ranks, pair_weight=pair_weight, pair_bias=pair_bias, score_weight=score_weight)


def reference(embeddings, ranks, pair_weight, pair_bias, score_weight):
    sorted_rows = jnp.zeros_like(embeddings).at[ranks].set(embeddings)
    padded = jnp.concatenate([sorted_rows, jnp.zeros((WIN - 1, E), embeddings.dtype)], axis=0)
    leading = sorted_rows.astype(jnp.float32)
    positions = jnp.arange(NTOTAL, dtype=jnp.int32)

    def one_offset(offset):
        partner = lax.dynamic_slice_in_dim(padded, offset, NTOTAL, 0).astype(jnp.float32)
        product = (leading * partner).astype(jnp.bfloat16)
        distance = jnp.abs(leading - partner).astype(jnp.bfloat16)
        features = jnp.concatenate([product, distance], axis=1)
        hidden = jnp.dot(features, pair_weight, preferred_element_type=jnp.float32) + pair_bias
        hidden = jax.nn.relu(hidden).astype(jnp.bfloat16)
        values = jnp.dot(hidden, score_weight, preferred_element_type=jnp.float32)
        return jnp.where(positions + offset < NTOTAL, values, jnp.zeros_like(values))

    offsets = jnp.arange(1, WIN, dtype=jnp.int32)
    return lax.map(one_offset, offsets)
```

```python
import functools

import jax
import jax.numpy as jnp
from jax import lax
from jax.experimental import pallas as pl
from jax.experimental.pallas import tpu as pltpu
from jax.sharding import PartitionSpec as P

MESH = pl.DeviceIdType.MESH
WIN = 32
ROWS = 1024
CAP = 16
NDEV = 128
UNITS = 16
STRIDE = ROWS // UNITS
GROUPS = 8
GROUP_DEVS = NDEV // GROUPS
GROUP_ROWS = GROUP_DEVS * CAP
CHUNK = 256
F32, BF16 = jnp.float32, jnp.bfloat16


def iota(shape, dim):
    return lax.broadcasted_iota(jnp.int32, shape, dim)


def one_hot(labels, rows):
    lanes = jnp.broadcast_to(labels, (rows, 128)).astype(BF16)
    numbers = iota((rows, 128), 0).astype(F32).astype(BF16)
    return jnp.where(numbers == lanes, jnp.ones((), BF16), jnp.zeros((), BF16))


def within(values, low, size):
    moved = values - low
    return jnp.where((moved >= 0) & (moved < size), moved, -1.0)


def kernel(
    ranks_ref, emb_ref, weight_ref, bias_ref, score_ref, out_ref,
    send_rows, recv_rows, send_pos, recv_pos, acc, tiles, shifted, halo_out, halo_in, score_mats, packed,
    send_sem, pos_send_sem, pos_recv_sem, halo_send_sem, halo_recv_sem, recv_sems,
):
    me = lax.axis_index("dev")
    my_z, my_x, my_y, my_c = me // 32, (me // 8) % 4, (me // 2) % 4, me % 2

    barrier = pltpu.get_barrier_semaphore()

    def greet(base, carry):
        for j in range(8):
            pl.semaphore_signal(barrier, inc=1, device_id=(base * 8 + j,), device_id_type=MESH)
        return carry

    lax.fori_loop(0, NDEV // 8, greet, 0)

    ranks = ranks_ref[...]
    owner = ranks // ROWS
    local = ranks - owner * ROWS
    rel = (
        ((owner // 32 - my_z) & 3) * 32
        + (((owner // 8) - my_x) & 3) * 8
        + (((owner // 2) - my_y) & 3) * 2
        + ((owner - my_c) & 1)
    )
    place = (local % STRIDE) * UNITS + local // STRIDE + 1
    rel_f = rel.astype(F32)
    place_high = (place // 32).astype(F32)
    place_low = (place % 32).astype(F32)
    members = [one_hot(rel_f[a : a + 1], NDEV) for a in range(8)]
    prefix = jnp.where(
        (iota((128, 256), 0) <= iota((128, 256), 1)), jnp.ones((), F32), jnp.zeros((), F32)
    ).astype(BF16)
    counts = jnp.dot(jnp.concatenate(members, axis=0), prefix, preferred_element_type=F32)
    base = jnp.zeros((128, 128), F32)
    slots = []
    for a in range(8):
        block = counts[a * 128 : (a + 1) * 128]
        mine = members[a].astype(F32) * (block[:, :128] + base)
        slots.append(jnp.sum(mine, axis=0, keepdims=True) - 1.0)
        base = base + block[:, 128:]
    slot = jnp.concatenate(slots, axis=0)

    lane_slot = (iota((128, 128), 0) % CAP).astype(F32).astype(BF16)
    tables = []
    for a in range(8):
        here = jnp.broadcast_to(slot[a : a + 1], (128, 128)).astype(BF16) == lane_slot
        zero = jnp.zeros((128, 128), BF16)
        tables.append(
            jnp.concatenate(
                [
                    jnp.where(here, jnp.broadcast_to(place_high[a : a + 1], (128, 128)).astype(BF16), zero),
                    jnp.where(here, jnp.broadcast_to(place_low[a : a + 1], (128, 128)).astype(BF16), zero),
                ],
                axis=0,
            )
        )
    digits = lax.dot_general(
        jnp.concatenate(members, axis=1),
        jnp.concatenate(tables, axis=1),
        (((1,), (1,)), ((), ())),
        preferred_element_type=F32,
    )
    send_pos[...] = digits[:, :128] * 32.0 + digits[:, 128:]

    target = rel_f * CAP + slot

    def pack(group, carry):
        labels = within(target, (group * GROUP_ROWS).astype(F32), GROUP_ROWS)
        choose = jnp.concatenate([one_hot(labels[a : a + 1], GROUP_ROWS) for a in range(8)], axis=1)
        rows = jnp.dot(choose, emb_ref[...], preferred_element_type=F32).astype(BF16)
        send_rows[pl.ds(pl.multiple_of(group * GROUP_ROWS, GROUP_ROWS), GROUP_ROWS), :] = rows
        return carry

    lax.fori_loop(0, GROUPS, pack, 0)

    columns = [((my_y + dy) % 4) * 2 + (my_c + dc) % 2 for dy in range(4) for dc in range(2)]

    def plane(step):
        return (((my_z + step // 4) % 4) * 4 + (my_x + step % 4) % 4) * 8

    def row_copy(step, j, base_id):
        part = pl.ds(pl.multiple_of((step * 8 + j) * CAP, CAP), CAP)
        return pltpu.make_async_remote_copy(
            src_ref=send_rows.at[part], dst_ref=recv_rows.at[part],
            send_sem=send_sem, recv_sem=recv_sems.at[step // 2],
            device_id=(base_id + columns[j],), device_id_type=MESH,
        )

    def pos_copy(step, j, base_id):
        part = pl.ds(step * 8 + j, 1)
        return pltpu.make_async_remote_copy(
            src_ref=send_pos.at[part], dst_ref=recv_pos.at[part],
            send_sem=pos_send_sem, recv_sem=pos_recv_sem,
            device_id=(base_id + columns[j],), device_id_type=MESH,
        )

    pl.semaphore_wait(barrier, NDEV)
    here = plane(0)
    for j in range(1, 8):
        pos_copy(0, j, here).start()
        row_copy(0, j, here).start()

    def send(step, carry):
        base_id = plane(step)
        for j in range(8):
            pos_copy(step, j, base_id).start()
            row_copy(step, j, base_id).start()
        return carry

    lax.fori_loop(1, 16, send, 0)

    recv_rows[:CAP, :] = send_rows[:CAP, :]
    recv_pos[0:1, :] = send_pos[0:1, :]

    column = jnp.transpose(jnp.broadcast_to(score_ref[...].astype(F32), (128, 128)))
    lane = iota((128, 128), 1)
    for k in range(WIN - 1):
        score_mats[k * 128 : (k + 1) * 128, :] = jnp.where(lane == k, column, 0.0).astype(BF16)

    rest = pl.ds(1, NDEV - 1)
    whole = pltpu.make_async_remote_copy(
        src_ref=send_pos.at[rest], dst_ref=recv_pos.at[rest], send_sem=pos_send_sem, recv_sem=pos_recv_sem,
        device_id=(me,), device_id_type=MESH,
    )
    whole.wait_send()
    whole.wait_recv()
    keep = (iota((NDEV, 128), 0) % 8) == (iota((NDEV, 128), 1) // CAP)
    wanted = jnp.sum(jnp.where(keep, recv_pos[...], 0.0).reshape(16, 8, 128), axis=1) - 1.0

    for group in range(GROUPS):
        first = CAP if group == 0 else group * GROUP_ROWS
        part = pl.ds(first, (group + 1) * GROUP_ROWS - first)
        pltpu.make_async_remote_copy(
            src_ref=send_rows.at[part], dst_ref=recv_rows.at[part],
            send_sem=send_sem, recv_sem=recv_sems.at[group], device_id=(me,), device_id_type=MESH,
        ).wait_recv()
        got = recv_rows[group * GROUP_ROWS : (group + 1) * GROUP_ROWS, :]
        for block in range(ROWS // CHUNK):
            labels = within(wanted[2 * group : 2 * group + 2], float(block * CHUNK), CHUNK)
            choose = jnp.concatenate([one_hot(labels[i : i + 1], CHUNK) for i in range(2)], axis=1)
            rows = jnp.dot(choose, got, preferred_element_type=F32)
            where = slice(block * CHUNK, (block + 1) * CHUNK)
            if group == 0:
                acc[where, :] = rows
            else:
                acc[where, :] = acc[where, :] + rows

    tiles[:ROWS, :] = acc[:ROWS, :].astype(BF16)

    halo_out[...] = acc[pl.ds(0, WIN, stride=UNITS), :].astype(BF16)
    before = lax.rem(me + NDEV - 1, NDEV)
    halo = pltpu.make_async_remote_copy(
        src_ref=halo_out, dst_ref=halo_in, send_sem=halo_send_sem, recv_sem=halo_recv_sem,
        device_id=(before,), device_id_type=MESH,
    )

    weight = weight_ref[...]
    bias = bias_ref[...]

    def score(chunk, carry):
        start = pl.multiple_of(chunk * CHUNK, CHUNK)
        leading = tiles[pl.ds(start, CHUNK), :]
        total = None
        for pair in range(WIN // 2):
            hiddens = []
            for k in (2 * pair + 1, 2 * pair + 2):
                if k == WIN:
                    continue
                partner = tiles[pl.ds(start + k * UNITS, CHUNK), :]
                features = jnp.concatenate([leading * partner, jnp.abs(leading - partner)], axis=1)
                hidden = jnp.dot(features, weight, preferred_element_type=F32) + bias
                hiddens.append(jnp.maximum(hidden.astype(BF16), jnp.zeros((), BF16)))
            hidden = jnp.concatenate(hiddens, axis=1) if len(hiddens) == 2 else hiddens[0]
            mats = score_mats[pair * 256 : pair * 256 + 128 * len(hiddens), :]
            term = jnp.dot(hidden, mats, preferred_element_type=F32)
            total = term if total is None else total + term
        packed[pl.ds(start, CHUNK), :] = total
        return carry

    halo.start()
    lax.fori_loop(0, 2, score, 0)
    halo.wait_send()
    halo.wait_recv()
    extra = (WIN - 1) * UNITS
    shifted[...] = acc[1 : 1 + extra + UNITS, :]
    shifted[pl.ds(UNITS - 1, WIN, stride=UNITS), :] = halo_in[...].astype(F32)
    tiles[ROWS : ROWS + extra, :] = shifted[:extra, :].astype(BF16)
    lax.fori_loop(2, 4, score, 0)

    offset = iota((WIN, 128), 0) + 1
    position = me * ROWS + iota((WIN, 128), 1)
    for block in range(8):
        rows = [packed[pl.ds(2 * block + i, STRIDE, stride=UNITS), :] for i in range(2)]
        turned = jnp.transpose(jnp.concatenate(rows, axis=0))[:WIN]
        inside = position + block * 128 + offset < NDEV * ROWS
        out_ref[:, block * 128 : (block + 1) * 128] = jnp.where(inside, turned, 0.0)[: WIN - 1]

    part = pl.ds(CAP, (NDEV - 1) * CAP)
    pltpu.make_async_remote_copy(
        src_ref=send_rows.at[part], dst_ref=recv_rows.at[part],
        send_sem=send_sem, recv_sem=recv_sems.at[0], device_id=(me,), device_id_type=MESH,
    ).wait_send()


def body(embeddings, ranks, pair_weight, pair_bias, score_weight):
    vmem = pl.BlockSpec(memory_space=pltpu.VMEM)
    return pl.pallas_call(
        kernel,
        out_shape=jax.ShapeDtypeStruct((WIN - 1, ROWS), F32),
        in_specs=[vmem] * 5,
        out_specs=vmem,
        scratch_shapes=[
            pltpu.VMEM((NDEV * CAP, 128), BF16),
            pltpu.VMEM((NDEV * CAP, 128), BF16),
            pltpu.VMEM((NDEV, 128), F32),
            pltpu.VMEM((NDEV, 128), F32),
            pltpu.VMEM((ROWS + 8, 128), F32),
            pltpu.VMEM((ROWS + WIN * UNITS, 128), BF16),
            pltpu.VMEM((WIN * UNITS, 128), F32),
            pltpu.VMEM((WIN, 128), BF16),
            pltpu.VMEM((WIN, 128), BF16),
            pltpu.VMEM((WIN * 128, 128), BF16),
            pltpu.VMEM((ROWS, 128), F32),
            pltpu.SemaphoreType.DMA,
            pltpu.SemaphoreType.DMA,
            pltpu.SemaphoreType.DMA,
            pltpu.SemaphoreType.DMA,
            pltpu.SemaphoreType.DMA,
            pltpu.SemaphoreType.DMA((GROUPS,)),
        ],
        compiler_params=pltpu.CompilerParams(collective_id=0, has_side_effects=True),
        name="neighborhood_scores",
    )(
        ranks.reshape(8, 128),
        embeddings,
        pair_weight,
        pair_bias.reshape(1, 128),
        score_weight.reshape(1, 128),
    )


def solution(mesh):
    placed = (P("dev", None), P("dev"), P(), P(), P())
    return jax.shard_map(
        body, mesh=mesh, in_specs=placed, out_specs=P(None, "dev"), check_vma=False
    )
```

```python
import functools

import jax
import jax.numpy as jnp
from jax import lax
from jax.experimental import pallas as pl
from jax.experimental.pallas import tpu as pltpu
from jax.sharding import PartitionSpec as P

MESH = pl.DeviceIdType.MESH
WIN = 32
ROWS = 1024
CAP = 16
NDEV = 128
UNITS = 16
STRIDE = ROWS // UNITS
GROUPS = 8
GROUP_DEVS = NDEV // GROUPS
GROUP_ROWS = GROUP_DEVS * CAP
CHUNK = 512
PLACES = 256
F32, BF16 = jnp.float32, jnp.bfloat16


def iota(shape, dim):
    return lax.broadcasted_iota(jnp.int32, shape, dim)


def one_hot(labels, rows):
    lanes = jnp.broadcast_to(labels, (rows, 128)).astype(BF16)
    numbers = iota((rows, 128), 0).astype(F32).astype(BF16)
    return jnp.where(numbers == lanes, jnp.ones((), BF16), jnp.zeros((), BF16))


def within(values, low, size):
    moved = values - low
    return jnp.where((moved >= 0) & (moved < size), moved, -1.0)


def kernel(
    ranks_ref, emb_hbm, weight_hbm, bias_ref, score_ref, out_ref,
    emb_ref, weight_ref, send_rows, recv_rows, send_pos, recv_pos, tiles, halo_out, halo_in, packed,
    load_sems, send_sem, pos_send_sem, pos_recv_sem, halo_send_sem, halo_recv_sem, recv_sems,
):
    me = lax.axis_index("dev")
    my_z, my_x, my_y, my_c = me // 32, (me // 8) % 4, (me // 2) % 4, me % 2

    load_emb = pltpu.make_async_copy(emb_hbm, emb_ref, load_sems.at[0])
    load_weight = pltpu.make_async_copy(weight_hbm, weight_ref, load_sems.at[1])
    load_emb.start()
    load_weight.start()
    barrier = pltpu.get_barrier_semaphore()

    def greet(base, carry):
        for j in range(8):
            pl.semaphore_signal(barrier, inc=1, device_id=(base * 8 + j,), device_id_type=MESH)
        return carry

    lax.fori_loop(0, NDEV // 8, greet, 0)

    ranks = ranks_ref[...]
    owner = ranks // ROWS
    local = ranks - owner * ROWS
    rel = (
        ((owner // 32 - my_z) & 3) * 32
        + (((owner // 8) - my_x) & 3) * 8
        + (((owner // 2) - my_y) & 3) * 2
        + ((owner - my_c) & 1)
    )
    place = (local % STRIDE) * UNITS + local // STRIDE + 1
    rel_f = rel.astype(F32)
    place_high = (place // 32).astype(F32)
    place_low = (place % 32).astype(F32)
    members = [one_hot(rel_f[a : a + 1], NDEV) for a in range(8)]
    prefix = jnp.where(
        (iota((128, 256), 0) <= iota((128, 256), 1)), jnp.ones((), F32), jnp.zeros((), F32)
    ).astype(BF16)
    counts = jnp.dot(jnp.concatenate(members, axis=0), prefix, preferred_element_type=F32)
    base = jnp.zeros((128, 128), F32)
    slots = []
    for a in range(8):
        block = counts[a * 128 : (a + 1) * 128]
        mine = members[a].astype(F32) * (block[:, :128] + base)
        slots.append(jnp.sum(mine, axis=0, keepdims=True) - 1.0)
        base = base + block[:, 128:]
    slot = jnp.concatenate(slots, axis=0)

    lane_slot = (iota((128, 128), 0) % CAP).astype(F32).astype(BF16)
    tables = []
    for a in range(8):
        here = jnp.broadcast_to(slot[a : a + 1], (128, 128)).astype(BF16) == lane_slot
        zero = jnp.zeros((128, 128), BF16)
        tables.append(
            jnp.concatenate(
                [
                    jnp.where(here, jnp.broadcast_to(place_high[a : a + 1], (128, 128)).astype(BF16), zero),
                    jnp.where(here, jnp.broadcast_to(place_low[a : a + 1], (128, 128)).astype(BF16), zero),
                ],
                axis=0,
            )
        )
    digits = lax.dot_general(
        jnp.concatenate(members, axis=1),
        jnp.concatenate(tables, axis=1),
        (((1,), (1,)), ((), ())),
        preferred_element_type=F32,
    )
    send_pos[...] = digits[:, :128] * 32.0 + digits[:, 128:]

    target = rel_f * CAP + slot

    load_emb.wait()
    emb = emb_ref[...]
    for group in range(GROUPS):
        labels = within(target, float(group * GROUP_ROWS), GROUP_ROWS)
        choose = jnp.concatenate([one_hot(labels[a : a + 1], GROUP_ROWS) for a in range(8)], axis=1)
        rows = jnp.dot(choose, emb, preferred_element_type=F32).astype(BF16)
        send_rows[group * GROUP_ROWS : (group + 1) * GROUP_ROWS, :] = rows

    columns = [((my_y + dy) % 4) * 2 + (my_c + dc) % 2 for dy in range(4) for dc in range(2)]

    def plane(step):
        return (((my_z + step // 4) % 4) * 4 + (my_x + step % 4) % 4) * 8

    def row_copy(step, j, base_id):
        part = pl.ds(pl.multiple_of((step * 8 + j) * CAP, CAP), CAP)
        return pltpu.make_async_remote_copy(
            src_ref=send_rows.at[part], dst_ref=recv_rows.at[part],
            send_sem=send_sem, recv_sem=recv_sems.at[step // 2],
            device_id=(base_id + columns[j],), device_id_type=MESH,
        )

    def pos_copy(step, j, base_id):
        part = pl.ds(step * 8 + j, 1)
        return pltpu.make_async_remote_copy(
            src_ref=send_pos.at[part], dst_ref=recv_pos.at[part],
            send_sem=pos_send_sem, recv_sem=pos_recv_sem,
            device_id=(base_id + columns[j],), device_id_type=MESH,
        )

    pl.semaphore_wait(barrier, NDEV)
    here = plane(0)
    for j in range(1, 8):
        pos_copy(0, j, here).start()
        row_copy(0, j, here).start()

    def send(step, carry):
        base_id = plane(step)
        for j in range(8):
            pos_copy(step, j, base_id).start()
            row_copy(step, j, base_id).start()
        return carry

    lax.fori_loop(1, 16, send, 0)

    recv_rows[:CAP, :] = send_rows[:CAP, :]
    recv_pos[0:1, :] = send_pos[0:1, :]

    rest = pl.ds(1, NDEV - 1)
    whole = pltpu.make_async_remote_copy(
        src_ref=send_pos.at[rest], dst_ref=recv_pos.at[rest], send_sem=pos_send_sem, recv_sem=pos_recv_sem,
        device_id=(me,), device_id_type=MESH,
    )
    whole.wait_send()
    whole.wait_recv()
    keep = (iota((NDEV, 128), 0) % 8) == (iota((NDEV, 128), 1) // CAP)
    wanted = jnp.sum(jnp.where(keep, recv_pos[...], 0.0).reshape(16, 8, 128), axis=1) - 1.0

    for group in range(GROUPS):
        first = CAP if group == 0 else group * GROUP_ROWS
        part = pl.ds(first, (group + 1) * GROUP_ROWS - first)
        pltpu.make_async_remote_copy(
            src_ref=send_rows.at[part], dst_ref=recv_rows.at[part],
            send_sem=send_sem, recv_sem=recv_sems.at[group], device_id=(me,), device_id_type=MESH,
        ).wait_recv()
        got = recv_rows[group * GROUP_ROWS : (group + 1) * GROUP_ROWS, :]
        for block in range(ROWS // PLACES):
            labels = within(wanted[2 * group : 2 * group + 2], float(block * PLACES), PLACES)
            choose = jnp.concatenate([one_hot(labels[i : i + 1], PLACES) for i in range(2)], axis=1)
            rows = jnp.dot(choose, got, preferred_element_type=F32)
            where = slice(block * PLACES, (block + 1) * PLACES)
            if group == 0:
                tiles[where, :] = rows
            else:
                tiles[where, :] = tiles[where, :] + rows

    halo_out[...] = tiles[pl.ds(0, WIN, stride=UNITS), :].astype(BF16)
    before = lax.rem(me + NDEV - 1, NDEV)
    halo = pltpu.make_async_remote_copy(
        src_ref=halo_out, dst_ref=halo_in, send_sem=halo_send_sem, recv_sem=halo_recv_sem,
        device_id=(before,), device_id_type=MESH,
    )

    load_weight.wait()
    weight = weight_ref[...]
    bias = bias_ref[...]
    score_weight = score_ref[...].astype(F32)

    def score(start):
        leading = tiles[start : start + CHUNK, :].astype(BF16)
        for k in range(1, WIN):
            partner = tiles[start + k * UNITS : start + k * UNITS + CHUNK, :].astype(BF16)
            features = jnp.concatenate([leading * partner, jnp.abs(leading - partner)], axis=1)
            hidden = jnp.dot(features, weight, preferred_element_type=F32) + bias
            hidden = jnp.maximum(hidden, 0.0)
            packed[start : start + CHUNK, k - 1 : k] = jnp.sum(hidden * score_weight, axis=1, keepdims=True)

    halo.start()
    score(0)
    halo.wait_send()
    halo.wait_recv()
    extra = (WIN - 1) * UNITS
    tiles[ROWS : ROWS + extra, :] = tiles[1 : 1 + extra, :]
    tiles[pl.ds(ROWS + UNITS - 1, WIN, stride=UNITS), :] = halo_in[...].astype(F32)
    score(CHUNK)

    offset = iota((WIN, 128), 0) + 1
    position = me * ROWS + iota((WIN, 128), 1)
    for block in range(8):
        rows = [packed[pl.ds(2 * block + i, STRIDE, stride=UNITS), :] for i in range(2)]
        turned = jnp.transpose(jnp.concatenate(rows, axis=0))[:WIN]
        inside = position + block * 128 + offset < NDEV * ROWS
        out_ref[:, block * 128 : (block + 1) * 128] = jnp.where(inside, turned, 0.0)[: WIN - 1]

    part = pl.ds(CAP, (NDEV - 1) * CAP)
    pltpu.make_async_remote_copy(
        src_ref=send_rows.at[part], dst_ref=recv_rows.at[part],
        send_sem=send_sem, recv_sem=recv_sems.at[0], device_id=(me,), device_id_type=MESH,
    ).wait_send()


def body(embeddings, ranks, pair_weight, pair_bias, score_weight):
    vmem = pl.BlockSpec(memory_space=pltpu.VMEM)
    hbm = pl.BlockSpec(memory_space=pl.ANY)
    return pl.pallas_call(
        kernel,
        out_shape=jax.ShapeDtypeStruct((WIN - 1, ROWS), F32),
        in_specs=[vmem, hbm, hbm, vmem, vmem],
        out_specs=vmem,
        scratch_shapes=[
            pltpu.VMEM((ROWS, 128), BF16),
            pltpu.VMEM((256, 128), BF16),
            pltpu.VMEM((NDEV * CAP, 128), BF16),
            pltpu.VMEM((NDEV * CAP, 128), BF16),
            pltpu.VMEM((NDEV, 128), F32),
            pltpu.VMEM((NDEV, 128), F32),
            pltpu.VMEM((ROWS + WIN * UNITS, 128), F32),
            pltpu.VMEM((WIN, 128), BF16),
            pltpu.VMEM((WIN, 128), BF16),
            pltpu.VMEM((ROWS, 128), F32),
            pltpu.SemaphoreType.DMA((2,)),
            pltpu.SemaphoreType.DMA,
            pltpu.SemaphoreType.DMA,
            pltpu.SemaphoreType.DMA,
            pltpu.SemaphoreType.DMA,
            pltpu.SemaphoreType.DMA,
            pltpu.SemaphoreType.DMA((GROUPS,)),
        ],
        compiler_params=pltpu.CompilerParams(collective_id=0, has_side_effects=True),
        name="neighborhood_scores",
    )(
        ranks.reshape(8, 128),
        embeddings,
        pair_weight,
        pair_bias.reshape(1, 128),
        score_weight.reshape(1, 128),
    )


def solution(mesh):
    placed = (P("dev", None), P("dev"), P(), P(), P())
    return jax.shard_map(
        body, mesh=mesh, in_specs=placed, out_specs=P(None, "dev"), check_vma=False
    )
```

```python
import functools

import jax
import jax.numpy as jnp
from jax import lax
from jax.experimental import pallas as pl
from jax.experimental.pallas import tpu as pltpu
from jax.sharding import PartitionSpec as P

MESH = pl.DeviceIdType.MESH
WIN = 32
ROWS = 1024
CAP = 16
NDEV = 128
UNITS = 16
STRIDE = ROWS // UNITS
GROUPS = 8
GROUP_DEVS = NDEV // GROUPS
GROUP_ROWS = GROUP_DEVS * CAP
CHUNK = 512
PLACES = 256
SPLIT = 7
F32, BF16 = jnp.float32, jnp.bfloat16


def iota(shape, dim):
    return lax.broadcasted_iota(jnp.int32, shape, dim)


def one_hot(labels, rows):
    lanes = jnp.broadcast_to(labels, (rows, 128)).astype(BF16)
    numbers = iota((rows, 128), 0).astype(F32).astype(BF16)
    return jnp.where(numbers == lanes, jnp.ones((), BF16), jnp.zeros((), BF16))


def within(values, low, size):
    moved = values - low
    return jnp.where((moved >= 0) & (moved < size), moved, -1.0)


def kernel(
    ranks_hbm, emb_hbm, weight_hbm, bias_hbm, score_hbm, out_ref,
    ranks_ref, emb_ref, weight_ref, bias_ref, score_ref,
    send_rows, recv_rows, send_pos, plane_pos, recv_pos, tiles, halo_out, halo_in, packed,
    load_sems, ready_sem, send_sem, plane_send_sem, plane_recv_sem, pos_send_sem, pos_recv_sem,
    halo_send_sem, halo_recv_sem, recv_sems,
):
    me = lax.axis_index("dev")
    my_z, my_x, my_y, my_c = me // 32, (me // 8) % 4, (me // 2) % 4, me % 2

    loads = [
        pltpu.make_async_copy(source, target, load_sems.at[i])
        for i, (source, target) in enumerate(
            [
                (ranks_hbm, ranks_ref), (emb_hbm, emb_ref), (weight_hbm, weight_ref),
                (bias_hbm, bias_ref), (score_hbm, score_ref),
            ]
        )
    ]
    for load in loads:
        load.start()

    columns = [((my_y + dy) % 4) * 2 + (my_c + dc) % 2 for dy in range(4) for dc in range(2)]

    def plane(step):
        step = (step * 5) % 16
        return (((my_z + step // 4) % 4) * 4 + (my_x + step % 4) % 4) * 8

    barrier = pltpu.get_barrier_semaphore()
    planes = [plane(step) for step in range(16)]
    plane_mates = [planes[step] + columns[0] for step in range(1, 16)]
    column_mates = [planes[0] + columns[j] for j in range(1, 8)]
    for mate in plane_mates + column_mates:
        pl.semaphore_signal(barrier, inc=1, device_id=(mate,), device_id_type=MESH)

    loads[0].wait()
    ranks = ranks_ref[...]
    owner = ranks // ROWS
    local = ranks - owner * ROWS
    plane_rel = ((owner // 32 - my_z) & 3) * 4 + ((owner // 8 - my_x) & 3)
    column_rel = ((owner // 2 - my_y) & 3) * 2 + ((owner - my_c) & 1)
    rel = ((plane_rel * 13) & 15) * 8 + column_rel
    place = (local % STRIDE) * UNITS + local // STRIDE + 1
    rel_f = rel.astype(F32)
    place_high = (place // 32).astype(F32)
    place_low = (place % 32).astype(F32)
    members = [one_hot(rel_f[a : a + 1], NDEV) for a in range(8)]
    prefix = jnp.where(
        (iota((128, 256), 0) <= iota((128, 256), 1)), jnp.ones((), F32), jnp.zeros((), F32)
    ).astype(BF16)
    counts = jnp.dot(jnp.concatenate(members, axis=0), prefix, preferred_element_type=F32)
    base = jnp.zeros((128, 128), F32)
    slots = []
    for a in range(8):
        block = counts[a * 128 : (a + 1) * 128]
        mine = members[a].astype(F32) * (block[:, :128] + base)
        slots.append(jnp.sum(mine, axis=0, keepdims=True) - 1.0)
        base = base + block[:, 128:]
    slot = jnp.concatenate(slots, axis=0)

    lane_slot = (iota((128, 128), 0) % CAP).astype(F32).astype(BF16)
    tables = []
    for a in range(8):
        here = jnp.broadcast_to(slot[a : a + 1], (128, 128)).astype(BF16) == lane_slot
        zero = jnp.zeros((128, 128), BF16)
        tables.append(
            jnp.concatenate(
                [
                    jnp.where(here, jnp.broadcast_to(place_high[a : a + 1], (128, 128)).astype(BF16), zero),
                    jnp.where(here, jnp.broadcast_to(place_low[a : a + 1], (128, 128)).astype(BF16), zero),
                ],
                axis=0,
            )
        )
    digits = lax.dot_general(
        jnp.concatenate(members, axis=1),
        jnp.concatenate(tables, axis=1),
        (((1,), (1,)), ((), ())),
        preferred_element_type=F32,
    )
    places = digits[:, :128] * 32.0 + digits[:, 128:]
    keep = (iota((NDEV, 128), 0) % 8) == (iota((NDEV, 128), 1) // CAP)
    by_step = jnp.sum(jnp.where(keep, places, 0.0).reshape(16, 8, 128), axis=1)
    send_pos[...] = by_step
    plane_pos[0:1, :] = by_step[0:1]

    pl.semaphore_wait(barrier, 22)
    for mate in column_mates:
        pl.semaphore_signal(ready_sem, inc=1, device_id=(mate,), device_id_type=MESH)
    for step in range(1, 16):
        pltpu.make_async_remote_copy(
            src_ref=send_pos.at[pl.ds(step, 1)], dst_ref=plane_pos.at[pl.ds(step, 1)],
            send_sem=plane_send_sem, recv_sem=plane_recv_sem,
            device_id=(plane_mates[step - 1],), device_id_type=MESH,
        ).start()

    target = rel_f * CAP + slot

    loads[1].wait()
    emb = emb_ref[...]
    for group in range(GROUPS):
        labels = within(target, float(group * GROUP_ROWS), GROUP_ROWS)
        choose = jnp.concatenate([one_hot(labels[a : a + 1], GROUP_ROWS) for a in range(8)], axis=1)
        rows = jnp.dot(choose, emb, preferred_element_type=F32).astype(BF16)
        send_rows[group * GROUP_ROWS : (group + 1) * GROUP_ROWS, :] = rows

    def row_copy(step, j, base_id):
        part = pl.ds(pl.multiple_of((step * 8 + j) * CAP, CAP), CAP)
        return pltpu.make_async_remote_copy(
            src_ref=send_rows.at[part], dst_ref=recv_rows.at[part],
            send_sem=send_sem, recv_sem=recv_sems.at[step // 2],
            device_id=(base_id + columns[j],), device_id_type=MESH,
        )

    def send(step, carry):
        base_id = plane(step)
        for j in range(8):
            row_copy(step, j, base_id).start()
        return carry

    pl.semaphore_wait(ready_sem, 7)
    for j in range(1, 8):
        row_copy(0, j, planes[0]).start()
    lax.fori_loop(1, SPLIT, send, 0)

    rest = pl.ds(1, 15)
    whole = pltpu.make_async_remote_copy(
        src_ref=send_pos.at[rest], dst_ref=plane_pos.at[rest],
        send_sem=plane_send_sem, recv_sem=plane_recv_sem, device_id=(me,), device_id_type=MESH,
    )
    whole.wait_send()
    whole.wait_recv()
    for j in range(1, 8):
        pltpu.make_async_remote_copy(
            src_ref=plane_pos, dst_ref=recv_pos.at[pl.ds(j * 16, 16)],
            send_sem=pos_send_sem, recv_sem=pos_recv_sem,
            device_id=(column_mates[j - 1],), device_id_type=MESH,
        ).start()
    lax.fori_loop(SPLIT, 16, send, 0)

    recv_rows[:CAP, :] = send_rows[:CAP, :]
    recv_pos[0:16, :] = plane_pos[...]

    rest = pl.ds(16, 112)
    whole = pltpu.make_async_remote_copy(
        src_ref=recv_pos.at[rest], dst_ref=recv_pos.at[rest],
        send_sem=pos_send_sem, recv_sem=pos_recv_sem, device_id=(me,), device_id_type=MESH,
    )
    whole.wait_send()
    whole.wait_recv()
    sender = iota((16, 128), 1) // CAP
    wanted = jnp.full((16, 128), -1.0, F32)
    for j in range(8):
        wanted = wanted + jnp.where(sender == j, recv_pos[j * 16 : (j + 1) * 16, :], 0.0)

    for group in range(GROUPS):
        first = CAP if group == 0 else group * GROUP_ROWS
        part = pl.ds(first, (group + 1) * GROUP_ROWS - first)
        pltpu.make_async_remote_copy(
            src_ref=send_rows.at[part], dst_ref=recv_rows.at[part],
            send_sem=send_sem, recv_sem=recv_sems.at[group], device_id=(me,), device_id_type=MESH,
        ).wait_recv()
        got = recv_rows[group * GROUP_ROWS : (group + 1) * GROUP_ROWS, :]
        for block in range(ROWS // PLACES):
            labels = within(wanted[2 * group : 2 * group + 2], float(block * PLACES), PLACES)
            choose = jnp.concatenate([one_hot(labels[i : i + 1], PLACES) for i in range(2)], axis=1)
            rows = jnp.dot(choose, got, preferred_element_type=F32)
            where = slice(block * PLACES, (block + 1) * PLACES)
            if group == 0:
                tiles[where, :] = rows
            else:
                tiles[where, :] = tiles[where, :] + rows

    halo_out[...] = tiles[pl.ds(0, WIN, stride=UNITS), :].astype(BF16)
    before = lax.rem(me + NDEV - 1, NDEV)
    halo = pltpu.make_async_remote_copy(
        src_ref=halo_out, dst_ref=halo_in, send_sem=halo_send_sem, recv_sem=halo_recv_sem,
        device_id=(before,), device_id_type=MESH,
    )

    for load in loads[2:]:
        load.wait()
    weight = weight_ref[...]
    bias = bias_ref[...]
    score_weight = score_ref[...].astype(F32)

    def score(start):
        leading = tiles[start : start + CHUNK, :].astype(BF16)
        for k in range(1, WIN):
            partner = tiles[start + k * UNITS : start + k * UNITS + CHUNK, :].astype(BF16)
            features = jnp.concatenate([leading * partner, jnp.abs(leading - partner)], axis=1)
            hidden = jnp.dot(features, weight, preferred_element_type=F32) + bias
            hidden = jnp.maximum(hidden, 0.0)
            packed[start : start + CHUNK, k - 1 : k] = jnp.sum(hidden * score_weight, axis=1, keepdims=True)

    halo.start()
    score(0)
    halo.wait_send()
    halo.wait_recv()
    extra = (WIN - 1) * UNITS
    tiles[ROWS : ROWS + extra, :] = tiles[1 : 1 + extra, :]
    tiles[pl.ds(ROWS + UNITS - 1, WIN, stride=UNITS), :] = halo_in[...].astype(F32)
    score(CHUNK)

    offset = iota((WIN, 128), 0) + 1
    position = me * ROWS + iota((WIN, 128), 1)
    for block in range(8):
        rows = [packed[pl.ds(2 * block + i, STRIDE, stride=UNITS), :] for i in range(2)]
        turned = jnp.transpose(jnp.concatenate(rows, axis=0))[:WIN]
        inside = position + block * 128 + offset < NDEV * ROWS
        out_ref[:, block * 128 : (block + 1) * 128] = jnp.where(inside, turned, 0.0)[: WIN - 1]

    part = pl.ds(CAP, (NDEV - 1) * CAP)
    pltpu.make_async_remote_copy(
        src_ref=send_rows.at[part], dst_ref=recv_rows.at[part],
        send_sem=send_sem, recv_sem=recv_sems.at[0], device_id=(me,), device_id_type=MESH,
    ).wait_send()


def body(embeddings, ranks, pair_weight, pair_bias, score_weight):
    vmem = pl.BlockSpec(memory_space=pltpu.VMEM)
    hbm = pl.BlockSpec(memory_space=pl.ANY)
    return pl.pallas_call(
        kernel,
        out_shape=jax.ShapeDtypeStruct((WIN - 1, ROWS), F32),
        in_specs=[hbm] * 5,
        out_specs=vmem,
        scratch_shapes=[
            pltpu.VMEM((8, 128), jnp.int32),
            pltpu.VMEM((ROWS, 128), BF16),
            pltpu.VMEM((256, 128), BF16),
            pltpu.VMEM((1, 128), F32),
            pltpu.VMEM((1, 128), BF16),
            pltpu.VMEM((NDEV * CAP, 128), BF16),
            pltpu.VMEM((NDEV * CAP, 128), BF16),
            pltpu.VMEM((16, 128), F32),
            pltpu.VMEM((16, 128), F32),
            pltpu.VMEM((NDEV, 128), F32),
            pltpu.VMEM((ROWS + WIN * UNITS, 128), F32),
            pltpu.VMEM((WIN, 128), BF16),
            pltpu.VMEM((WIN, 128), BF16),
            pltpu.VMEM((ROWS, 128), F32),
            pltpu.SemaphoreType.DMA((5,)),
            pltpu.SemaphoreType.REGULAR,
            pltpu.SemaphoreType.DMA,
            pltpu.SemaphoreType.DMA,
            pltpu.SemaphoreType.DMA,
            pltpu.SemaphoreType.DMA,
            pltpu.SemaphoreType.DMA,
            pltpu.SemaphoreType.DMA,
            pltpu.SemaphoreType.DMA,
            pltpu.SemaphoreType.DMA((GROUPS,)),
        ],
        compiler_params=pltpu.CompilerParams(collective_id=0, has_side_effects=True),
        name="neighborhood_scores",
    )(
        ranks.reshape(8, 128),
        embeddings,
        pair_weight,
        pair_bias.reshape(1, 128),
        score_weight.reshape(1, 128),
    )


def solution(mesh):
    placed = (P("dev", None), P("dev"), P(), P(), P())
    return jax.shard_map(
        body, mesh=mesh, in_specs=placed, out_specs=P(None, "dev"), check_vma=False
    )
```

```python
import functools

import jax
import jax.numpy as jnp
from jax import lax
from jax.experimental import pallas as pl
from jax.experimental.pallas import tpu as pltpu
from jax.sharding import PartitionSpec as P

MESH = pl.DeviceIdType.MESH
WIN = 32
ROWS = 1024
CAP = 16
NDEV = 128
UNITS = 16
STRIDE = ROWS // UNITS
GROUPS = 8
GROUP_DEVS = NDEV // GROUPS
GROUP_ROWS = GROUP_DEVS * CAP
CHUNK = 512
PLACES = 256
SPLIT = 12
SELF = NDEV - 1


def hops(steps):
    return min(steps, 4 - steps)


PLANES = sorted(range(16), key=lambda q: -hops(q // 4) - hops(q % 4))
COLUMNS = sorted(range(8), key=lambda q: -2 * hops(q // 2) - q % 2)
F32, BF16 = jnp.float32, jnp.bfloat16


def iota(shape, dim):
    return lax.broadcasted_iota(jnp.int32, shape, dim)


def one_hot(labels, rows):
    lanes = jnp.broadcast_to(labels, (rows, 128)).astype(BF16)
    numbers = iota((rows, 128), 0).astype(F32).astype(BF16)
    return jnp.where(numbers == lanes, jnp.ones((), BF16), jnp.zeros((), BF16))


def lookup(values, order):
    return sum(jnp.where(values == q, jnp.int32(i), jnp.int32(0)) for i, q in enumerate(order) if i)


def within(values, low, size):
    moved = values - low
    return jnp.where((moved >= 0) & (moved < size), moved, -1.0)


def kernel(
    ranks_hbm, emb_hbm, weight_hbm, bias_hbm, score_hbm, out_ref,
    ranks_ref, emb_ref, weight_ref, bias_ref, score_ref,
    send_rows, recv_rows, send_pos, plane_pos, recv_pos, tiles, halo_out, halo_in, packed,
    load_sems, ready_sem, send_sem, plane_send_sem, plane_recv_sem, pos_send_sem, pos_recv_sem,
    halo_send_sem, halo_recv_sem, recv_sems,
):
    me = lax.axis_index("dev")
    my_z, my_x, my_y, my_c = me // 32, (me // 8) % 4, (me // 2) % 4, me % 2

    loads = [
        pltpu.make_async_copy(source, target, load_sems.at[i])
        for i, (source, target) in enumerate(
            [
                (ranks_hbm, ranks_ref), (emb_hbm, emb_ref), (weight_hbm, weight_ref),
                (bias_hbm, bias_ref), (score_hbm, score_ref),
            ]
        )
    ]
    for load in loads:
        load.start()

    planes = [((my_z + q // 4) % 4) * 32 + ((my_x + q % 4) % 4) * 8 for q in PLANES]
    columns = [((my_y + q // 2) % 4) * 2 + (my_c + q % 2) % 2 for q in COLUMNS]

    barrier = pltpu.get_barrier_semaphore()
    plane_mates = [planes[step] + columns[7] for step in range(15)]
    column_mates = [planes[15] + columns[j] for j in range(7)]
    for mate in plane_mates + column_mates:
        pl.semaphore_signal(barrier, inc=1, device_id=(mate,), device_id_type=MESH)

    loads[0].wait()
    ranks = ranks_ref[...]
    owner = ranks // ROWS
    local = ranks - owner * ROWS
    plane_rel = ((owner // 32 - my_z) & 3) * 4 + ((owner // 8 - my_x) & 3)
    column_rel = ((owner // 2 - my_y) & 3) * 2 + ((owner - my_c) & 1)
    rel = lookup(plane_rel, PLANES) * 8 + lookup(column_rel, COLUMNS)
    place = (local % STRIDE) * UNITS + local // STRIDE + 1
    rel_f = rel.astype(F32)
    place_high = (place // 32).astype(F32)
    place_low = (place % 32).astype(F32)
    members = [one_hot(rel_f[a : a + 1], NDEV) for a in range(8)]
    prefix = jnp.where(
        (iota((128, 256), 0) <= iota((128, 256), 1)), jnp.ones((), F32), jnp.zeros((), F32)
    ).astype(BF16)
    counts = jnp.dot(jnp.concatenate(members, axis=0), prefix, preferred_element_type=F32)
    base = jnp.zeros((128, 128), F32)
    slots = []
    for a in range(8):
        block = counts[a * 128 : (a + 1) * 128]
        mine = members[a].astype(F32) * (block[:, :128] + base)
        slots.append(jnp.sum(mine, axis=0, keepdims=True) - 1.0)
        base = base + block[:, 128:]
    slot = jnp.concatenate(slots, axis=0)

    lane_slot = (iota((128, 128), 0) % CAP).astype(F32).astype(BF16)
    tables = []
    for a in range(8):
        here = jnp.broadcast_to(slot[a : a + 1], (128, 128)).astype(BF16) == lane_slot
        zero = jnp.zeros((128, 128), BF16)
        tables.append(
            jnp.concatenate(
                [
                    jnp.where(here, jnp.broadcast_to(place_high[a : a + 1], (128, 128)).astype(BF16), zero),
                    jnp.where(here, jnp.broadcast_to(place_low[a : a + 1], (128, 128)).astype(BF16), zero),
                ],
                axis=0,
            )
        )
    digits = lax.dot_general(
        jnp.concatenate(members, axis=1),
        jnp.concatenate(tables, axis=1),
        (((1,), (1,)), ((), ())),
        preferred_element_type=F32,
    )
    places = digits[:, :128] * 32.0 + digits[:, 128:]
    keep = (iota((NDEV, 128), 0) % 8) == (iota((NDEV, 128), 1) // CAP)
    by_step = jnp.sum(jnp.where(keep, places, 0.0).reshape(16, 8, 128), axis=1)
    send_pos[...] = by_step
    plane_pos[15:16, :] = by_step[15:16]

    target = rel_f * CAP + slot

    loads[1].wait()
    emb = emb_ref[...]
    for group in range(GROUPS):
        labels = within(target, float(group * GROUP_ROWS), GROUP_ROWS)
        choose = jnp.concatenate([one_hot(labels[a : a + 1], GROUP_ROWS) for a in range(8)], axis=1)
        rows = jnp.dot(choose, emb, preferred_element_type=F32).astype(BF16)
        send_rows[group * GROUP_ROWS : (group + 1) * GROUP_ROWS, :] = rows

    recv_rows[SELF * CAP :, :] = send_rows[SELF * CAP :, :]

    def send(step, j):
        part = pl.ds((step * 8 + j) * CAP, CAP)
        pltpu.make_async_remote_copy(
            src_ref=send_rows.at[part], dst_ref=recv_rows.at[part],
            send_sem=send_sem, recv_sem=recv_sems.at[step // 2],
            device_id=(planes[step] + columns[j],), device_id_type=MESH,
        ).start()

    pl.semaphore_wait(barrier, 22)
    for mate in column_mates:
        pl.semaphore_signal(ready_sem, inc=1, device_id=(mate,), device_id_type=MESH)
    for step in range(15):
        send(step, 7)
    for j in range(7):
        send(15, j)
    for step in range(15):
        pltpu.make_async_remote_copy(
            src_ref=send_pos.at[pl.ds(step, 1)], dst_ref=plane_pos.at[pl.ds(step, 1)],
            send_sem=plane_send_sem, recv_sem=plane_recv_sem,
            device_id=(plane_mates[step],), device_id_type=MESH,
        ).start()
    pl.semaphore_wait(ready_sem, 7)
    for step in range(SPLIT):
        for j in range(7):
            send(step, j)

    rest = pl.ds(0, 15)
    whole = pltpu.make_async_remote_copy(
        src_ref=send_pos.at[rest], dst_ref=plane_pos.at[rest],
        send_sem=plane_send_sem, recv_sem=plane_recv_sem, device_id=(me,), device_id_type=MESH,
    )
    whole.wait_send()
    whole.wait_recv()
    for j in range(7):
        pltpu.make_async_remote_copy(
            src_ref=plane_pos, dst_ref=recv_pos.at[pl.ds(j * 16, 16)],
            send_sem=pos_send_sem, recv_sem=pos_recv_sem,
            device_id=(column_mates[j],), device_id_type=MESH,
        ).start()
    for step in range(SPLIT, 15):
        for j in range(7):
            send(step, j)

    recv_pos[112:, :] = plane_pos[...]

    rest = pl.ds(0, 112)
    whole = pltpu.make_async_remote_copy(
        src_ref=recv_pos.at[rest], dst_ref=recv_pos.at[rest],
        send_sem=pos_send_sem, recv_sem=pos_recv_sem, device_id=(me,), device_id_type=MESH,
    )
    whole.wait_send()
    whole.wait_recv()
    sender = iota((16, 128), 1) // CAP
    wanted = jnp.full((16, 128), -1.0, F32)
    for j in range(8):
        wanted = wanted + jnp.where(sender == j, recv_pos[j * 16 : (j + 1) * 16, :], 0.0)

    per = GROUPS // 4
    for part in range(4):
        for group in range(part * per, (part + 1) * per):
            first = group * GROUP_ROWS
            arriving = pl.ds(first, min(first + GROUP_ROWS, SELF * CAP) - first)
            pltpu.make_async_remote_copy(
                src_ref=send_rows.at[arriving], dst_ref=recv_rows.at[arriving],
                send_sem=send_sem, recv_sem=recv_sems.at[group], device_id=(me,), device_id_type=MESH,
            ).wait_recv()
        got = recv_rows[part * per * GROUP_ROWS : (part + 1) * per * GROUP_ROWS, :]
        for block in range(ROWS // PLACES):
            labels = within(wanted[2 * part * per : 2 * (part + 1) * per], float(block * PLACES), PLACES)
            choose = jnp.concatenate([one_hot(labels[i : i + 1], PLACES) for i in range(2 * per)], axis=1)
            rows = jnp.dot(choose, got, preferred_element_type=F32)
            where = slice(block * PLACES, (block + 1) * PLACES)
            if part == 0:
                tiles[where, :] = rows
            else:
                tiles[where, :] = tiles[where, :] + rows

    halo_out[...] = tiles[pl.ds(0, WIN, stride=UNITS), :].astype(BF16)
    before = lax.rem(me + NDEV - 1, NDEV)
    halo = pltpu.make_async_remote_copy(
        src_ref=halo_out, dst_ref=halo_in, send_sem=halo_send_sem, recv_sem=halo_recv_sem,
        device_id=(before,), device_id_type=MESH,
    )

    for load in loads[2:]:
        load.wait()
    weight = weight_ref[...]
    bias = bias_ref[...]
    score_weight = score_ref[...].astype(F32)

    def score(start):
        leading = tiles[start : start + CHUNK, :].astype(BF16)
        for k in range(1, WIN):
            partner = tiles[start + k * UNITS : start + k * UNITS + CHUNK, :].astype(BF16)
            features = jnp.concatenate([leading * partner, jnp.abs(leading - partner)], axis=1)
            hidden = jnp.dot(features, weight, preferred_element_type=F32) + bias
            hidden = jnp.maximum(hidden, 0.0)
            packed[start : start + CHUNK, k - 1 : k] = jnp.sum(hidden * score_weight, axis=1, keepdims=True)

    halo.start()
    score(0)
    halo.wait_send()
    halo.wait_recv()
    extra = (WIN - 1) * UNITS
    tiles[ROWS : ROWS + extra, :] = tiles[1 : 1 + extra, :]
    tiles[pl.ds(ROWS + UNITS - 1, WIN, stride=UNITS), :] = halo_in[...].astype(F32)
    score(CHUNK)

    offset = iota((WIN, 128), 0) + 1
    position = me * ROWS + iota((WIN, 128), 1)
    for block in range(8):
        rows = [packed[pl.ds(2 * block + i, STRIDE, stride=UNITS), :] for i in range(2)]
        turned = jnp.transpose(jnp.concatenate(rows, axis=0))[:WIN]
        inside = position + block * 128 + offset < NDEV * ROWS
        out_ref[:, block * 128 : (block + 1) * 128] = jnp.where(inside, turned, 0.0)[: WIN - 1]

    part = pl.ds(0, SELF * CAP)
    pltpu.make_async_remote_copy(
        src_ref=send_rows.at[part], dst_ref=recv_rows.at[part],
        send_sem=send_sem, recv_sem=recv_sems.at[0], device_id=(me,), device_id_type=MESH,
    ).wait_send()


def body(embeddings, ranks, pair_weight, pair_bias, score_weight):
    vmem = pl.BlockSpec(memory_space=pltpu.VMEM)
    hbm = pl.BlockSpec(memory_space=pl.ANY)
    return pl.pallas_call(
        kernel,
        out_shape=pltpu.VMEM((WIN - 1, ROWS), F32),
        in_specs=[hbm] * 5,
        out_specs=vmem,
        scratch_shapes=[
            pltpu.VMEM((8, 128), jnp.int32),
            pltpu.VMEM((ROWS, 128), BF16),
            pltpu.VMEM((256, 128), BF16),
            pltpu.VMEM((1, 128), F32),
            pltpu.VMEM((1, 128), BF16),
            pltpu.VMEM((NDEV * CAP, 128), BF16),
            pltpu.VMEM((NDEV * CAP, 128), BF16),
            pltpu.VMEM((16, 128), F32),
            pltpu.VMEM((16, 128), F32),
            pltpu.VMEM((NDEV, 128), F32),
            pltpu.VMEM((ROWS + WIN * UNITS, 128), F32),
            pltpu.VMEM((WIN, 128), BF16),
            pltpu.VMEM((WIN, 128), BF16),
            pltpu.VMEM((ROWS, 128), F32),
            pltpu.SemaphoreType.DMA((5,)),
            pltpu.SemaphoreType.REGULAR,
            pltpu.SemaphoreType.DMA,
            pltpu.SemaphoreType.DMA,
            pltpu.SemaphoreType.DMA,
            pltpu.SemaphoreType.DMA,
            pltpu.SemaphoreType.DMA,
            pltpu.SemaphoreType.DMA,
            pltpu.SemaphoreType.DMA,
            pltpu.SemaphoreType.DMA((GROUPS,)),
        ],
        compiler_params=pltpu.CompilerParams(collective_id=0, has_side_effects=True),
        name="neighborhood_scores",
    )(
        ranks.reshape(8, 128),
        embeddings,
        pair_weight,
        pair_bias.reshape(1, 128),
        score_weight.reshape(1, 128),
    )


def solution(mesh):
    placed = (P("dev", None), P("dev"), P(), P(), P())
    return jax.shard_map(
        body, mesh=mesh, in_specs=placed, out_specs=P(None, "dev"), check_vma=False
    )
```

```python
import functools

import jax
import jax.numpy as jnp
from jax import lax
from jax.experimental import pallas as pl
from jax.experimental.pallas import tpu as pltpu
from jax.sharding import PartitionSpec as P

MESH = pl.DeviceIdType.MESH
WIN = 32
ROWS = 1024
CAP = 16
NDEV = 128
UNITS = 16
STRIDE = ROWS // UNITS
GROUPS = 8
GROUP_DEVS = NDEV // GROUPS
GROUP_ROWS = GROUP_DEVS * CAP
CHUNK = 512
PLACES = 256
SPLIT = 12
SELF = NDEV - 1


def hops(steps):
    return min(steps, 4 - steps)


PLANES = sorted(range(16), key=lambda q: -hops(q // 4) - hops(q % 4))
COLUMNS = sorted(range(8), key=lambda q: -2 * hops(q // 2) - q % 2)
F32, BF16 = jnp.float32, jnp.bfloat16


def iota(shape, dim):
    return lax.broadcasted_iota(jnp.int32, shape, dim)


def one_hot(labels, rows):
    lanes = jnp.broadcast_to(labels, (rows, 128)).astype(BF16)
    numbers = iota((rows, 128), 0).astype(F32).astype(BF16)
    return jnp.where(numbers == lanes, jnp.ones((), BF16), jnp.zeros((), BF16))


def lookup(values, order):
    return sum(jnp.where(values == q, jnp.int32(i), jnp.int32(0)) for i, q in enumerate(order) if i)


def within(values, low, size):
    moved = values - low
    return jnp.where((moved >= 0) & (moved < size), moved, -1.0)


def kernel(
    ranks_hbm, emb_hbm, weight_hbm, bias_hbm, score_hbm, out_ref,
    ranks_ref, emb_ref, weight_ref, bias_ref, score_ref,
    send_rows, recv_rows, send_pos, plane_pos, recv_pos, tiles, halo_out, halo_in, packed,
    load_sems, ready_sem, send_sem, plane_send_sem, plane_recv_sem, pos_send_sem, pos_recv_sem,
    halo_send_sem, halo_recv_sem, recv_sems,
):
    me = lax.axis_index("dev")
    my_z, my_x, my_y, my_c = me // 32, (me // 8) % 4, (me // 2) % 4, me % 2

    loads = [
        pltpu.make_async_copy(source, target, load_sems.at[i])
        for i, (source, target) in enumerate(
            [
                (ranks_hbm, ranks_ref), (emb_hbm, emb_ref), (weight_hbm, weight_ref),
                (bias_hbm, bias_ref), (score_hbm, score_ref),
            ]
        )
    ]
    for load in loads:
        load.start()

    planes = [((my_z + q // 4) % 4) * 32 + ((my_x + q % 4) % 4) * 8 for q in PLANES]
    columns = [((my_y + q // 2) % 4) * 2 + (my_c + q % 2) % 2 for q in COLUMNS]

    barrier = pltpu.get_barrier_semaphore()
    plane_mates = [planes[step] + columns[7] for step in range(15)]
    column_mates = [planes[15] + columns[j] for j in range(7)]
    for mate in plane_mates + column_mates:
        pl.semaphore_signal(barrier, inc=1, device_id=(mate,), device_id_type=MESH)

    loads[0].wait()
    ranks = ranks_ref[...]
    owner = ranks // ROWS
    local = ranks - owner * ROWS
    plane_rel = ((owner // 32 - my_z) & 3) * 4 + ((owner // 8 - my_x) & 3)
    column_rel = ((owner // 2 - my_y) & 3) * 2 + ((owner - my_c) & 1)
    rel = lookup(plane_rel, PLANES) * 8 + lookup(column_rel, COLUMNS)
    place = (local % STRIDE) * UNITS + local // STRIDE + 1
    rel_f = rel.astype(F32)
    place_high = (place // 32).astype(F32)
    place_low = (place % 32).astype(F32)
    members = [one_hot(rel_f[a : a + 1], NDEV) for a in range(8)]
    prefix = jnp.where(
        (iota((128, 256), 0) <= iota((128, 256), 1)), jnp.ones((), F32), jnp.zeros((), F32)
    ).astype(BF16)
    counts = jnp.dot(jnp.concatenate(members, axis=0), prefix, preferred_element_type=F32)
    base = jnp.zeros((128, 128), F32)
    slots = []
    for a in range(8):
        block = counts[a * 128 : (a + 1) * 128]
        mine = members[a].astype(F32) * (block[:, :128] + base)
        slots.append(jnp.sum(mine, axis=0, keepdims=True) - 1.0)
        base = base + block[:, 128:]
    slot = jnp.concatenate(slots, axis=0)

    lane_slot = (iota((128, 128), 0) % CAP).astype(F32).astype(BF16)
    tables = []
    for a in range(8):
        here = jnp.broadcast_to(slot[a : a + 1], (128, 128)).astype(BF16) == lane_slot
        zero = jnp.zeros((128, 128), BF16)
        tables.append(
            jnp.concatenate(
                [
                    jnp.where(here, jnp.broadcast_to(place_high[a : a + 1], (128, 128)).astype(BF16), zero),
                    jnp.where(here, jnp.broadcast_to(place_low[a : a + 1], (128, 128)).astype(BF16), zero),
                ],
                axis=0,
            )
        )
    digits = lax.dot_general(
        jnp.concatenate(members, axis=1),
        jnp.concatenate(tables, axis=1),
        (((1,), (1,)), ((), ())),
        preferred_element_type=F32,
    )
    places = digits[:, :128] * 32.0 + digits[:, 128:]
    keep = (iota((NDEV, 128), 0) % 8) == (iota((NDEV, 128), 1) // CAP)
    by_step = jnp.sum(jnp.where(keep, places, 0.0).reshape(16, 8, 128), axis=1)
    send_pos[...] = by_step
    plane_pos[15:16, :] = by_step[15:16]

    target = rel_f * CAP + slot

    loads[1].wait()
    emb = emb_ref[...]
    for group in range(GROUPS):
        labels = within(target, float(group * GROUP_ROWS), GROUP_ROWS)
        choose = jnp.concatenate([one_hot(labels[a : a + 1], GROUP_ROWS) for a in range(8)], axis=1)
        rows = jnp.dot(choose, emb, preferred_element_type=F32).astype(BF16)
        send_rows[group * GROUP_ROWS : (group + 1) * GROUP_ROWS, :] = rows

    recv_rows[SELF * CAP :, :] = send_rows[SELF * CAP :, :]

    def send(step, j):
        part = pl.ds((step * 8 + j) * CAP, CAP)
        pltpu.make_async_remote_copy(
            src_ref=send_rows.at[part], dst_ref=recv_rows.at[part],
            send_sem=send_sem, recv_sem=recv_sems.at[step // 2],
            device_id=(planes[step] + columns[j],), device_id_type=MESH,
        ).start()

    pl.semaphore_wait(barrier, 22)
    for mate in column_mates:
        pl.semaphore_signal(ready_sem, inc=1, device_id=(mate,), device_id_type=MESH)
    for step in range(15):
        send(step, 7)
    for j in range(7):
        send(15, j)
    for step in range(15):
        pltpu.make_async_remote_copy(
            src_ref=send_pos.at[pl.ds(step, 1)], dst_ref=plane_pos.at[pl.ds(step, 1)],
            send_sem=plane_send_sem, recv_sem=plane_recv_sem,
            device_id=(plane_mates[step],), device_id_type=MESH,
        ).start()
    pl.semaphore_wait(ready_sem, 7)
    for step in range(SPLIT):
        for j in range(7):
            send(step, j)

    rest = pl.ds(0, 15)
    whole = pltpu.make_async_remote_copy(
        src_ref=send_pos.at[rest], dst_ref=plane_pos.at[rest],
        send_sem=plane_send_sem, recv_sem=plane_recv_sem, device_id=(me,), device_id_type=MESH,
    )
    whole.wait_send()
    whole.wait_recv()
    for j in range(7):
        pltpu.make_async_remote_copy(
            src_ref=plane_pos, dst_ref=recv_pos.at[pl.ds(j * 16, 16)],
            send_sem=pos_send_sem, recv_sem=pos_recv_sem,
            device_id=(column_mates[j],), device_id_type=MESH,
        ).start()
    for step in range(SPLIT, 15):
        for j in range(7):
            send(step, j)

    recv_pos[112:, :] = plane_pos[...]

    rest = pl.ds(0, 112)
    whole = pltpu.make_async_remote_copy(
        src_ref=recv_pos.at[rest], dst_ref=recv_pos.at[rest],
        send_sem=pos_send_sem, recv_sem=pos_recv_sem, device_id=(me,), device_id_type=MESH,
    )
    whole.wait_send()
    whole.wait_recv()
    sender = iota((16, 128), 1) // CAP
    wanted = jnp.full((16, 128), -1.0, F32)
    for j in range(8):
        wanted = wanted + jnp.where(sender == j, recv_pos[j * 16 : (j + 1) * 16, :], 0.0)

    per = GROUPS // 4
    for part in range(4):
        for group in range(part * per, (part + 1) * per):
            first = group * GROUP_ROWS
            arriving = pl.ds(first, min(first + GROUP_ROWS, SELF * CAP) - first)
            pltpu.make_async_remote_copy(
                src_ref=send_rows.at[arriving], dst_ref=recv_rows.at[arriving],
                send_sem=send_sem, recv_sem=recv_sems.at[group], device_id=(me,), device_id_type=MESH,
            ).wait_recv()
        got = recv_rows[part * per * GROUP_ROWS : (part + 1) * per * GROUP_ROWS, :]
        for block in range(ROWS // PLACES):
            labels = within(wanted[2 * part * per : 2 * (part + 1) * per], float(block * PLACES), PLACES)
            choose = jnp.concatenate([one_hot(labels[i : i + 1], PLACES) for i in range(2 * per)], axis=1)
            rows = jnp.dot(choose, got, preferred_element_type=F32)
            where = slice(block * PLACES, (block + 1) * PLACES)
            if part == 0:
                tiles[where, :] = rows
            else:
                tiles[where, :] = tiles[where, :] + rows

    halo_out[...] = tiles[pl.ds(0, WIN, stride=UNITS), :].astype(BF16)
    before = lax.rem(me + NDEV - 1, NDEV)
    halo = pltpu.make_async_remote_copy(
        src_ref=halo_out, dst_ref=halo_in, send_sem=halo_send_sem, recv_sem=halo_recv_sem,
        device_id=(before,), device_id_type=MESH,
    )

    for load in loads[2:]:
        load.wait()
    weight = weight_ref[...]
    bias = bias_ref[...]
    score_weight = score_ref[...].astype(F32)

    def score(start):
        leading = tiles[start : start + CHUNK, :].astype(BF16)
        for k in range(1, WIN):
            partner = tiles[start + k * UNITS : start + k * UNITS + CHUNK, :].astype(BF16)
            features = jnp.concatenate([leading * partner, jnp.abs(leading - partner)], axis=1)
            hidden = jnp.dot(features, weight, preferred_element_type=F32) + bias
            hidden = jnp.maximum(hidden, 0.0)
            packed[start : start + CHUNK, k - 1 : k] = jnp.sum(hidden * score_weight, axis=1, keepdims=True)

    halo.start()
    score(0)
    halo.wait_send()
    halo.wait_recv()
    extra = (WIN - 1) * UNITS
    tiles[ROWS : ROWS + extra, :] = tiles[1 : 1 + extra, :]
    tiles[pl.ds(ROWS + UNITS - 1, WIN, stride=UNITS), :] = halo_in[...].astype(F32)
    score(CHUNK)

    offset = iota((WIN, 128), 0) + 1
    position = me * ROWS + iota((WIN, 128), 1)
    for block in range(8):
        rows = [packed[pl.ds(2 * block + i, STRIDE, stride=UNITS), :] for i in range(2)]
        turned = jnp.transpose(jnp.concatenate(rows, axis=0))[:WIN]
        inside = position + block * 128 + offset < NDEV * ROWS
        out_ref[:, block * 128 : (block + 1) * 128] = jnp.where(inside, turned, 0.0)[: WIN - 1]

    part = pl.ds(0, SELF * CAP)
    pltpu.make_async_remote_copy(
        src_ref=send_rows.at[part], dst_ref=recv_rows.at[part],
        send_sem=send_sem, recv_sem=recv_sems.at[0], device_id=(me,), device_id_type=MESH,
    ).wait_send()


def body(embeddings, ranks, pair_weight, pair_bias, score_weight):
    vmem = pl.BlockSpec(memory_space=pltpu.VMEM)
    hbm = pl.BlockSpec(memory_space=pl.ANY)
    return pl.pallas_call(
        kernel,
        out_shape=pltpu.VMEM((WIN - 1, ROWS), F32),
        in_specs=[hbm] * 5,
        out_specs=vmem,
        scratch_shapes=[
            pltpu.VMEM((8, 128), jnp.int32),
            pltpu.VMEM((ROWS, 128), BF16),
            pltpu.VMEM((256, 128), BF16),
            pltpu.VMEM((1, 128), F32),
            pltpu.VMEM((1, 128), BF16),
            pltpu.VMEM((NDEV * CAP, 128), BF16),
            pltpu.VMEM((NDEV * CAP, 128), BF16),
            pltpu.VMEM((16, 128), F32),
            pltpu.VMEM((16, 128), F32),
            pltpu.VMEM((NDEV, 128), F32),
            pltpu.VMEM((ROWS + (WIN + 1) * UNITS, 128), F32),
            pltpu.VMEM((WIN, 128), BF16),
            pltpu.VMEM((WIN, 128), BF16),
            pltpu.VMEM((ROWS + UNITS, 128), F32),
            pltpu.SemaphoreType.DMA((5,)),
            pltpu.SemaphoreType.REGULAR,
            pltpu.SemaphoreType.DMA,
            pltpu.SemaphoreType.DMA,
            pltpu.SemaphoreType.DMA,
            pltpu.SemaphoreType.DMA,
            pltpu.SemaphoreType.DMA,
            pltpu.SemaphoreType.DMA,
            pltpu.SemaphoreType.DMA,
            pltpu.SemaphoreType.DMA((GROUPS,)),
        ],
        compiler_params=pltpu.CompilerParams(collective_id=0, has_side_effects=True),
        name="neighborhood_scores",
    )(
        ranks.reshape(8, 128),
        embeddings,
        pair_weight,
        pair_bias.reshape(1, 128),
        score_weight.reshape(1, 128),
    )


def solution(mesh):
    placed = (P("dev", None), P("dev"), P(), P(), P())
    return jax.shard_map(
        body, mesh=mesh, in_specs=placed, out_specs=P(None, "dev"), check_vma=False
    )
```
